128 devices in a mesh: mod: 2 (over y_hi), exp: 64 (over z, y_lo, x, core).
Axes of the slice: x: 4, y: 4 (y_hi: 2, y_lo: 2; y = y_hi * 2 + y_lo), z: 4, core: 2. Of those that a mesh axis runs over, the one named last changes fastest.
Arguments:
- tokens: bfloat16 [2, 32768, 1024], P('mod', 'exp'), may hold values from -60 to 60
- bottleneck: bfloat16 [256, 4, 1024], P('exp'), may hold values from -6 to 6
- clip_ids: int32 [2, 32768], P('mod', 'exp'), may hold values from 0 to 255, as said below
- expert_ids: int32 [2, 32768], P('mod', 'exp'), may hold values from 0 to 63, as said below
- slots: int32 [2, 32768], P('mod', 'exp'), may hold values from 0 to 31, as said below
- norm1_gain: bfloat16 [2, 1024], P('mod'), may hold values from 0.099609375 to 1.8984375
- attn_qkv: bfloat16 [2, 1024, 3072], P('mod'), may hold values from -2 to 2
- attn_out: bfloat16 [2, 1024, 1024], P('mod'), may hold values from -0.1875 to 0.1875
- norm2_gain: bfloat16 [2, 1024], P('mod'), may hold values from 0.099609375 to 1.8984375
- router: bfloat16 [1024, 64], replicated, may hold values from -0.1875 to 0.1875
- fc_in: bfloat16 [64, 1024, 4096], P('exp'), may hold values from -0.1875 to 0.1875
- fc_out: bfloat16 [64, 4096, 1024], P('exp'), may hold values from -0.09375 to 0.09375
Outputs:
- mixed_tokens: bfloat16 [2, 32768, 1024], P('mod', 'exp')
- new_bottleneck: bfloat16 [256, 4, 1024], P('exp')
The draws below stay inside these ranges and needn't reach their ends.
Inputs may be any that keep to these rules, and one draw needn't show every extreme that they name: `clip_ids`: Non-decreasing in each modality; the tokens of block b of 512 rows belong to clips b * 4 to (b + 1) * 4 - 1, each of which has one or more of them. `expert_ids`: each token's single expert. For the k tokens of one block of 512 rows of one modality that share an expert, the slots are 0 to k - 1 in some order; k is at most 32; in every block of each modality one expert, the same for all blocks of that modality, has k = 32.
All inputs are finite; a program needn't handle non-finite values.
Results may differ from the reference program's by a relative error of at most 0.0085.
Values may be sent and summed in bfloat16 or wider, within the bound.
A program may use at most 128 MiB of HBM per device.

```python
import math
import jax
import jax.numpy as jnp
from jax import lax

D = 1024
FF = 4096
HEAD = 64
NB = 4
TOK_DEV = 512
CLIPS_DEV = 4
EXPERTS = 64
TOKENS = 32768
CLIPS = 256
CAP = 16


def routing_table(key):
    blocks = TOKENS // TOK_DEV
    queue_len = 2 * CAP
    seat_count = EXPERTS * queue_len
    routing_key = jax.random.fold_in(key, 7001)
    hot_key, level_key, block_key = jax.random.split(routing_key, 3)
    hottest = jax.random.randint(hot_key, (2,), 0, EXPERTS)
    levels = jax.random.randint(level_key, (2, EXPERTS), 0, 4)
    block_seeds = jax.random.split(block_key, 2 * blocks)
    modality_of = jnp.arange(2 * blocks, dtype=jnp.int32) // blocks
    seat_index = jnp.arange(seat_count, dtype=jnp.int32)
    seat_expert = seat_index // queue_len

    def one_block(block_seed, modality):
        second_key, noise_key, order_key = jax.random.split(block_seed, 3)
        second = jax.random.randint(second_key, (), 0, EXPERTS)
        jitter = jax.random.randint(noise_key, (seat_count,), 0, 4096)
        favoured = (seat_expert == hottest[modality]) | (seat_expert == second)
        seat_score = jitter + levels[modality][seat_expert] * 1024 + jnp.where(favoured, 16384, 0)
        ranked = seat_score * seat_count + seat_index
        picked = lax.top_k(ranked, TOK_DEV)[1]
        marked = jnp.zeros((seat_count,), jnp.int32).at[picked].set(1)
        grouped = marked.reshape(EXPERTS, queue_len)
        rank_table = (jnp.cumsum(grouped, axis=1) - grouped).reshape(seat_count)
        token_order = jax.random.permutation(order_key, TOK_DEV)
        assigned = picked[token_order]
        return (seat_expert[assigned], rank_table[assigned])
    experts_drawn, slots_drawn = jax.vmap(one_block)(block_seeds, modality_of)
    return (experts_drawn.reshape(2, TOKENS).astype(jnp.int32), slots_drawn.reshape(2, TOKENS).astype(jnp.int32))


def draw_expert_ids(key, part):
    return routing_table(key)[0]


def draw_slots(key, part):
    return routing_table(key)[1]


def draw_clip_ids(key, part):
    blocks = TOKENS // TOK_DEV
    block_seeds = jax.random.split(jax.random.fold_in(key, 7002), 2 * blocks)
    position = jnp.arange(TOK_DEV, dtype=jnp.int32)

    def one_block(block_seed):
        cuts = jax.random.permutation(block_seed, TOK_DEV - 1)[:CLIPS_DEV - 1] + 1
        return jnp.sum((position[:, None] >= cuts[None, :]).astype(jnp.int32), axis=1)
    local_ids = jax.vmap(one_block)(block_seeds).reshape(2, blocks, TOK_DEV)
    offsets = jnp.arange(blocks, dtype=jnp.int32)[None, :, None] * CLIPS_DEV
    return (local_ids + offsets).reshape(2, TOKENS).astype(jnp.int32)


def draw_tokens(key, part):
    normal_draw = jnp.clip(jax.random.normal(key, (2, TOKENS, D), jnp.float32), -6.0, 6.0)
    return normal_draw.astype(jnp.bfloat16)


def draw_attn_qkv(key, part):
    unit_scale = 1.0 / math.sqrt(D)
    entries = jax.random.normal(key, (2, D, 3 * D), jnp.float32) * unit_scale
    return jnp.clip(entries, -2.0, 2.0).astype(jnp.bfloat16)


def shard_levels(stream_key, shape, pieces, smallest, top_value):
    gain = 1.0
    for dim, parts in pieces:
        steps = jax.random.uniform(jax.random.fold_in(jax.random.fold_in(stream_key, 6), dim), (parts,), jnp.float32, smallest / len(pieces), top_value / len(pieces))
        gain = gain * jnp.repeat(jnp.exp(steps), shape[dim] // parts).reshape((-1,) + (1,) * (len(shape) - 1 - dim))
    return gain


def scatter_about(stream_key, shape, scale, limit, cuts=(), kind=jnp.bfloat16):
    factor_of = shard_levels(stream_key, shape, cuts, -0.22, 0.18) if cuts else 1.0
    values = jax.random.normal(stream_key, shape, jnp.float32) * scale * factor_of
    return jnp.minimum(jnp.maximum(values, -limit), limit).astype(kind)


def setup_inputs(seed: int = 0) -> dict:
    key_list = jax.random.split(jax.random.key(seed), 13)
    return {
        "tokens": draw_tokens(jax.random.fold_in(key_list[12], 71), 0),
        "bottleneck": scatter_about(key_list[1], (CLIPS, NB, D), 1.0, 6.0, ((0, 64),)),
        "clip_ids": draw_clip_ids(jax.random.fold_in(key_list[12], 71), 0),
        "expert_ids": draw_expert_ids(jax.random.fold_in(key_list[12], 71), 0),
        "slots": draw_slots(jax.random.fold_in(key_list[12], 71), 0),
        "norm1_gain": jnp.clip(1.0 + 0.18 * jax.random.normal(key_list[5], (2, D), jnp.float32), 0.099609375, 1.8984375).astype(jnp.bfloat16),
        "attn_qkv": draw_attn_qkv(jax.random.fold_in(key_list[12], 71), 0),
        "attn_out": scatter_about(key_list[7], (2, D, D), D ** -0.5, 0.1875, ((0, 2),)),
        "norm2_gain": jnp.clip(1.0 + 0.18 * jax.random.normal(key_list[8], (2, D), jnp.float32), 0.099609375, 1.8984375).astype(jnp.bfloat16),
        "router": scatter_about(key_list[9], (D, EXPERTS), D ** -0.5, 0.1875),
        "fc_in": scatter_about(key_list[10], (EXPERTS, D, FF), D ** -0.5, 0.1875, ((0, 64),)),
        "fc_out": scatter_about(key_list[11], (EXPERTS, FF, D), FF ** -0.5, 0.09375, ((0, 64),)),
    }


EPSILON = 1e-06

def layer_norm(features, scales):
    row_mean = lax.optimization_barrier(jnp.mean(features, axis=-1, keepdims=True))
    centred = features - row_mean
    spread = lax.optimization_barrier(jnp.mean(centred * centred, axis=-1, keepdims=True))
    return centred * lax.rsqrt(spread + EPSILON) * scales.astype(jnp.float32)

def attend(token_rows, latent_rows, token_clip, clip_start, scales, w_qkv, w_out):
    n_clips, n_latent, model_width = latent_rows.shape
    n_tokens = token_rows.shape[0]
    all_rows = jnp.concatenate([token_rows, latent_rows.reshape(n_clips * n_latent, model_width)], axis=0)
    row_count = all_rows.shape[0]
    head_count = model_width // HEAD
    normed = layer_norm(all_rows.astype(jnp.float32), scales).astype(jnp.bfloat16)
    packed = jnp.dot(normed, w_qkv, preferred_element_type=jnp.float32).astype(jnp.bfloat16)
    queries = packed[:, :model_width].reshape(row_count, head_count, HEAD)
    key_rows = packed[:, model_width:2 * model_width].reshape(row_count, head_count, HEAD)
    value_rows = packed[:, 2 * model_width:].reshape(row_count, head_count, HEAD)
    latent_clip = clip_start + jnp.arange(n_clips * n_latent, dtype=jnp.int32) // n_latent
    row_clip = jnp.concatenate([token_clip.astype(jnp.int32), latent_clip.astype(jnp.int32)])
    allowed = row_clip[:, None] == row_clip[None, :]
    scores = jnp.einsum('qhd,khd->hqk', queries.astype(jnp.float32), key_rows.astype(jnp.float32)) * (1.0 / math.sqrt(HEAD))
    scores = jnp.where(allowed[None, :, :], scores, -jnp.inf)
    row_max = lax.optimization_barrier(jnp.max(scores, axis=-1, keepdims=True))
    weights = jnp.exp(scores - row_max)
    attn_weights = (weights / lax.optimization_barrier(jnp.sum(weights, axis=-1, keepdims=True))).astype(jnp.bfloat16)
    attended = jnp.einsum('hqk,khd->qhd', attn_weights.astype(jnp.float32), value_rows.astype(jnp.float32))
    attended = attended.reshape(row_count, model_width).astype(jnp.bfloat16)
    updated = all_rows.astype(jnp.float32) + jnp.dot(attended, w_out, preferred_element_type=jnp.float32)
    return (updated[:n_tokens], updated[n_tokens:].reshape(n_clips, n_latent, model_width))

def expert_step(operands):
    block_rows, weight_in, weight_out = operands
    hidden_units = jnp.dot(block_rows, weight_in, preferred_element_type=jnp.float32)
    activated = jax.nn.gelu(hidden_units, approximate=False).astype(jnp.bfloat16)
    return jnp.dot(activated, weight_out, preferred_element_type=jnp.float32).astype(jnp.bfloat16)

def reference(tokens, bottleneck, clip_ids, expert_ids, slots, norm1_gain, attn_qkv, attn_out, norm2_gain, router, fc_in, fc_out):
    model_width = tokens.shape[-1]
    blocks = tokens.shape[1] // TOK_DEV
    latent = bottleneck.reshape(blocks, CLIPS_DEV, NB, model_width)
    starts = jnp.arange(blocks, dtype=jnp.int32) * CLIPS_DEV
    block_of = jnp.arange(blocks * TOK_DEV, dtype=jnp.int32) // TOK_DEV
    column = jnp.arange(EXPERTS, dtype=jnp.int32)
    slot_total = EXPERTS * blocks * CAP
    outputs = []
    latents = []
    for modality in range(2):

        def one_block(operands):
            token_rows, latent_rows, token_clip, clip_start = operands
            return attend(token_rows, latent_rows, token_clip, clip_start, norm1_gain[modality], attn_qkv[modality], attn_out[modality])
        mid_tokens, mid_latent = lax.map(one_block, (tokens[modality].reshape(blocks, TOK_DEV, model_width), latent, clip_ids[modality].reshape(blocks, TOK_DEV), starts))
        mid_tokens = mid_tokens.reshape(blocks * TOK_DEV, model_width)
        latents.append(mid_latent)
        expert_in = layer_norm(mid_tokens, norm2_gain[modality]).astype(jnp.bfloat16)
        logits = jnp.dot(expert_in, router, preferred_element_type=jnp.float32)
        chosen = expert_ids[modality].astype(jnp.int32)
        slot_ids = slots[modality].astype(jnp.int32)
        picked = lax.optimization_barrier(jnp.sum(jnp.where(column[None, :] == chosen[:, None], logits, jnp.zeros_like(logits)), axis=1))
        gate_value = jax.nn.sigmoid(picked)
        served = slot_ids < CAP
        position = jnp.where(served, chosen * (blocks * CAP) + block_of * CAP + slot_ids, slot_total).astype(jnp.int32)
        buffer = jnp.zeros((slot_total, model_width), jnp.bfloat16).at[position].set(expert_in, mode='drop')
        served_rows = lax.map(expert_step, (buffer.reshape(EXPERTS, blocks * CAP, model_width), fc_in, fc_out))
        served_rows = served_rows.reshape(slot_total, model_width)
        returned = jnp.take(served_rows, position, axis=0, mode='fill', fill_value=0)
        outputs.append((mid_tokens + gate_value[:, None] * returned.astype(jnp.float32)).astype(jnp.bfloat16))
    mixed_tokens = jnp.stack(outputs)
    new_bottleneck = ((latents[0] + latents[1]) * 0.5).astype(jnp.bfloat16).reshape(blocks * CLIPS_DEV, NB, model_width)
    return (mixed_tokens, new_bottleneck)
```

```python
import functools
import math

import jax
import jax.numpy as jnp
from jax import lax
from jax.experimental import pallas as pl
from jax.experimental.pallas import tpu as pltpu
from jax.sharding import PartitionSpec as P

MESH = pl.DeviceIdType.MESH
EPSILON = 1e-06
BIG = 2.0**100
F32 = jnp.float32
BF16 = jnp.bfloat16

T = 512
L = 16
R = T + L
KEYS = 640
D = 1024
FF = 4096
CAP = 16
EXPERTS = 64
GROUPS = 4
ORDER = (2, 1, 3, 0)
FF_TILE = 512


def dot(a, b):
    return lax.dot_general(a, b, (((1,), (0,)), ((), ())), preferred_element_type=F32)


def dot_nt(a, b):
    return lax.dot_general(a, b, (((1,), (1,)), ((), ())), preferred_element_type=F32)


def norm_rows(rows, gain):
    mean = jnp.mean(rows, axis=-1, keepdims=True)
    centred = rows - mean
    spread = jnp.mean(centred * centred, axis=-1, keepdims=True)
    return centred * lax.rsqrt(spread + EPSILON) * gain


def column_of(row):
    eye = lax.broadcasted_iota(jnp.int32, (128, 128), 0) == lax.broadcasted_iota(
        jnp.int32, (128, 128), 1
    )
    pieces = []
    for i in range(row.shape[1] // 128):
        block = jnp.broadcast_to(row[:, i * 128 : (i + 1) * 128], (128, 128))
        pieces.append(jnp.sum(jnp.where(eye, block, 0.0), axis=1, keepdims=True))
    return jnp.concatenate(pieces, axis=0)


def layer_kernel(
    tok, lat, clip, eid, slot, g1, g2, router, wqkv_hbm, wout_hbm, fin_hbm, fout_hbm,
    out, newb,
    wqkv, wout, fin, fout, latx, normed, packed, qmask, kmask, attended, mid, expert_in,
    gate, disp, recv, outb, ret, acc, lat_send, lat_recv,
    wsem, dsend, drecv, rsend, rrecv, lsem,
):
    m = lax.axis_index("mod")
    e = lax.axis_index("exp")
    me = lax.rem(e, 16)
    z = e // 16
    y = me // 8
    x = lax.rem(me // 2, 4)
    c = lax.rem(me, 2)

    def partner(r):
        return (
            lax.rem(y + r // 8, 2) * 8
            + lax.rem(x + lax.rem(r // 2, 4), 4) * 2
            + lax.rem(c + r, 2)
        )

    qkv_copies = []
    for i in range(3):
        cols = pl.ds(i * D, D)
        cp = pltpu.make_async_copy(wqkv_hbm.at[0, :, cols], wqkv.at[:, cols], wsem.at[i])
        cp.start()
        qkv_copies.append(cp)
    out_copy = pltpu.make_async_copy(wout_hbm.at[0], wout, wsem.at[3])
    fin_copy = pltpu.make_async_copy(fin_hbm.at[0], fin, wsem.at[4])
    fout_copy = pltpu.make_async_copy(fout_hbm.at[0], fout, wsem.at[5])

    barrier = pltpu.get_barrier_semaphore()
    pl.semaphore_signal(barrier, inc=1, device_id=(1 - m, e), device_id_type=MESH)
    for g in range(GROUPS):
        zz = lax.rem(z + g, 4) * 16

        def greet(r, carry, zz=zz):
            pl.semaphore_signal(
                barrier, inc=1, device_id=(m, zz + partner(r)), device_id_type=MESH
            )
            return carry

        lax.fori_loop(1 if g == 0 else 0, 16, greet, 0)

    clip_start = e * 4
    lane = lax.broadcasted_iota(jnp.int32, (T, 128), 1)
    clip_col = column_of((clip[...] - clip_start).astype(F32)).astype(jnp.int32)
    hit = lane == clip_col
    qmask[0:T, :] = jnp.where(hit | (lane == 4), -BIG, 0.0).astype(BF16)
    kmask[0:T, :] = jnp.where(hit | (lane >= 4), 0.0, 1.0).astype(BF16)
    lane_l = lax.broadcasted_iota(jnp.int32, (L, 128), 1)
    clip_l = lax.broadcasted_iota(jnp.int32, (L, 128), 0) // 4
    hit_l = lane_l == clip_l
    qmask[T:R, :] = jnp.where(hit_l | (lane_l == 4), -BIG, 0.0).astype(BF16)
    kmask[T:R, :] = jnp.where(hit_l | (lane_l >= 4), 0.0, 1.0).astype(BF16)
    lane_p = lax.broadcasted_iota(jnp.int32, (KEYS - R, 128), 1)
    kmask[R:KEYS, :] = jnp.where(lane_p == 4, 1.0, 0.0).astype(BF16)
    packed[R:KEYS, :] = jnp.zeros((KEYS - R, 3 * D), BF16)

    gain1 = g1[...].astype(F32)

    def norm1(i, carry):
        rows = pl.ds(pl.multiple_of(i * 32, 32), 32)
        normed[rows, :] = norm_rows(tok[0, rows, :].astype(F32), gain1).astype(BF16)
        return carry

    lax.fori_loop(0, T // 32, norm1, 0)
    for i in range(4):
        latx[4 * i : 4 * i + 4, :] = lat[i].astype(F32)
    normed[T:R, :] = norm_rows(latx[...], gain1).astype(BF16)

    for i in range(3):
        qkv_copies[i].wait()
        if i == 0:
            out_copy.start()

        def project(j, carry, i=i):
            cols = pl.ds(pl.multiple_of(i * D + j * 512, 512), 512)
            piece = dot(normed[...], wqkv[:, cols]).astype(BF16)
            if i == 0:
                piece = piece * (1.0 / 8.0)
            packed[0:R, cols] = piece.astype(BF16)
            return carry

        lax.fori_loop(0, 2, project, 0)
    fin_copy.start()
    fout_copy.start()

    def pair(p, carry):
        col = pl.multiple_of(p * 128, 128)
        keys = jnp.concatenate([packed[:, pl.ds(D + col, 128)], kmask[...]], axis=1)
        values = jnp.concatenate(
            [packed[:, pl.ds(2 * D + col, 128)], jnp.ones((KEYS, 128), BF16)], axis=1
        )
        for row0 in range(0, R, 176):
            queries = packed[row0 : row0 + 176, pl.ds(col, 128)]
            first = lax.broadcasted_iota(jnp.int32, (176, 128), 1) < 64
            heads = []
            for half in range(2):
                mine = jnp.where(first if half == 0 else ~first, queries, jnp.zeros_like(queries))
                q = jnp.concatenate([mine, qmask[row0 : row0 + 176, :]], axis=1)
                s = dot_nt(q, keys)
                top = jnp.max(s, axis=-1, keepdims=True)
                w = jnp.exp(s - top).astype(BF16)
                o = dot(w, values)
                heads.append(o[:, :128] / o[:, 128:])
            attended[row0 : row0 + 176, pl.ds(col, 128)] = jnp.where(
                first, heads[0], heads[1]
            ).astype(BF16)
        return carry

    lax.fori_loop(0, D // 128, pair, 0)

    out_copy.wait()

    def project_out(j, carry):
        cols = pl.ds(pl.multiple_of(j * 512, 512), 512)
        mid[:, cols] = dot(attended[...], wout[:, cols])
        return carry

    lax.fori_loop(0, 2, project_out, 0)

    gain2 = g2[...].astype(F32)

    def norm2(i, carry):
        rows = pl.ds(pl.multiple_of(i * 32, 32), 32)
        updated = mid[rows, :] + tok[0, rows, :].astype(F32)
        mid[rows, :] = updated
        expert_in[rows, :] = norm_rows(updated, gain2).astype(BF16)
        return carry

    lax.fori_loop(0, T // 32, norm2, 0)
    lat_send[...] = (mid[T:R, :] + latx[...]).astype(BF16)

    pos_row = jnp.where(slot[...] < CAP, eid[...] * CAP + slot[...], -1)
    pl.semaphore_wait(barrier, 64)
    lat_copy = pltpu.make_async_remote_copy(
        src_ref=lat_send, dst_ref=lat_recv, send_sem=lsem.at[0], recv_sem=lsem.at[1],
        device_id=(1 - m, e), device_id_type=MESH,
    )
    lat_copy.start()
    for g in ORDER:
        zz = lax.rem(z + g, 4)
        place = lax.broadcasted_iota(jnp.int32, (256, T), 0) + zz * 256
        onehot = jnp.where(place == pos_row, 1.0, 0.0).astype(BF16)
        disp[g] = dot(onehot, expert_in[...]).astype(BF16).reshape(16, CAP, D)

        def send(r, carry, g=g, zz=zz):
            j = partner(r)
            pltpu.make_async_remote_copy(
                src_ref=disp.at[g, j], dst_ref=recv.at[g, me],
                send_sem=dsend.at[g], recv_sem=drecv.at[g],
                device_id=(m, zz * 16 + j), device_id_type=MESH,
            ).start()
            return carry

        lax.fori_loop(1 if g == 0 else 0, 16, send, 0)
    recv[0, me] = disp[0, me]

    logits = dot(expert_in[...], router[...])
    eid_col = column_of(eid[...].astype(F32)).astype(jnp.int32)
    expert_lane = lax.broadcasted_iota(jnp.int32, (T, EXPERTS), 1)
    picked = jnp.sum(jnp.where(expert_lane == eid_col, logits, 0.0), axis=1, keepdims=True)
    gate[...] = 1.0 / (1.0 + jnp.exp(-picked))
    pos_col = column_of(pos_row.astype(F32)).astype(jnp.int32)

    fin_copy.wait()
    fout_copy.wait()
    for g in ORDER:
        n = 15 if g == 0 else 16
        zz = lax.rem(z + 4 - g, 4)
        landed = recv.at[g, pl.ds(0, n)]
        pltpu.make_async_copy(landed, landed, drecv.at[g]).wait()
        rows_in = recv[g].reshape(256, D)
        acc[...] = jnp.zeros_like(acc)

        def expert(f, carry, rows_in=rows_in):
            cols = pl.ds(pl.multiple_of(f * FF_TILE, FF_TILE), FF_TILE)
            h = dot(rows_in, fin[:, cols])
            h = (0.5 * h * (1.0 + lax.erf(h * math.sqrt(0.5)))).astype(BF16)
            acc[...] += dot(h, fout[cols, :])
            return carry

        lax.fori_loop(0, FF // FF_TILE, expert, 0)
        outb[g] = acc[...].astype(BF16).reshape(16, CAP, D)

        def send_back(r, carry, g=g, zz=zz):
            j = partner(r)
            pltpu.make_async_remote_copy(
                src_ref=outb.at[g, j], dst_ref=ret.at[g, me],
                send_sem=rsend.at[g], recv_sem=rrecv.at[g],
                device_id=(m, zz * 16 + j), device_id_type=MESH,
            ).start()
            return carry

        lax.fori_loop(1 if g == 0 else 0, 16, send_back, 0)
        if g == 0:
            ret[0, me] = outb[0, me]

    lat_copy.wait()
    both = (lat_send[...].astype(F32) + lat_recv[...].astype(F32)) * 0.5
    for i in range(4):
        newb[i] = both[4 * i : 4 * i + 4, :].astype(BF16)

    for k, g in enumerate(ORDER):
        n = 15 if g == 0 else 16
        zz = lax.rem(z + g, 4)
        landed = ret.at[g, pl.ds(0, n)]
        pltpu.make_async_copy(landed, landed, rrecv.at[g]).wait()
        place = lax.broadcasted_iota(jnp.int32, (T, 256), 1) + zz * 256
        onehot = jnp.where(place == pos_col, 1.0, 0.0).astype(BF16)
        total = mid[0:T, :] + gate[...] * dot(onehot, ret[g].reshape(256, D))
        if k < GROUPS - 1:
            mid[0:T, :] = total
        else:
            out[0] = total.astype(BF16)

    for g in range(GROUPS):
        n = 15 if g == 0 else 16
        sent = disp.at[g, pl.ds(0, n)]
        pltpu.make_async_copy(sent, sent, dsend.at[g]).wait()
        sent = outb.at[g, pl.ds(0, n)]
        pltpu.make_async_copy(sent, sent, rsend.at[g]).wait()


def on_device(
    tokens, bottleneck, clip_ids, expert_ids, slots, norm1_gain, attn_qkv, attn_out,
    norm2_gain, router, fc_in, fc_out,
):
    vmem = pl.BlockSpec(memory_space=pltpu.VMEM)
    hbm = pl.BlockSpec(memory_space=pl.ANY)
    dma = pltpu.SemaphoreType.DMA
    return pl.pallas_call(
        layer_kernel,
        out_shape=(
            jax.ShapeDtypeStruct(tokens.shape, BF16),
            jax.ShapeDtypeStruct(bottleneck.shape, BF16),
        ),
        in_specs=[vmem] * 8 + [hbm] * 4,
        out_specs=(vmem, vmem),
        scratch_shapes=[
            pltpu.VMEM((D, 3 * D), BF16),
            pltpu.VMEM((D, D), BF16),
            pltpu.VMEM((D, FF), BF16),
            pltpu.VMEM((FF, D), BF16),
            pltpu.VMEM((L, D), F32),
            pltpu.VMEM((R, D), BF16),
            pltpu.VMEM((KEYS, 3 * D), BF16),
            pltpu.VMEM((R, 128), BF16),
            pltpu.VMEM((KEYS, 128), BF16),
            pltpu.VMEM((R, D), BF16),
            pltpu.VMEM((R, D), F32),
            pltpu.VMEM((T, D), BF16),
            pltpu.VMEM((T, 1), F32),
            pltpu.VMEM((GROUPS, 16, CAP, D), BF16),
            pltpu.VMEM((GROUPS, 16, CAP, D), BF16),
            pltpu.VMEM((GROUPS, 16, CAP, D), BF16),
            pltpu.VMEM((GROUPS, 16, CAP, D), BF16),
            pltpu.VMEM((256, D), F32),
            pltpu.VMEM((L, D), BF16),
            pltpu.VMEM((L, D), BF16),
            dma((6,)),
            dma((GROUPS,)),
            dma((GROUPS,)),
            dma((GROUPS,)),
            dma((GROUPS,)),
            dma((2,)),
        ],
        compiler_params=pltpu.CompilerParams(
            collective_id=0, has_side_effects=True, vmem_limit_bytes=62 * 2**20
        ),
    )(
        tokens, bottleneck, clip_ids, expert_ids, slots, norm1_gain, norm2_gain, router,
        attn_qkv, attn_out, fc_in, fc_out,
    )


def solution(mesh):
    in_specs = (
        P("mod", "exp", None),
        P("exp", None, None),
        P("mod", "exp"),
        P("mod", "exp"),
        P("mod", "exp"),
        P("mod", None),
        P("mod", None, None),
        P("mod", None, None),
        P("mod", None),
        P(),
        P("exp", None, None),
        P("exp", None, None),
    )
    out_specs = (P("mod", "exp", None), P("exp", None, None))
    return jax.shard_map(
        on_device, mesh=mesh, in_specs=in_specs, out_specs=out_specs, check_vma=False
    )
```

```python
import functools
import math

import jax
import jax.numpy as jnp
from jax import lax
from jax.experimental import pallas as pl
from jax.experimental.pallas import tpu as pltpu
from jax.sharding import PartitionSpec as P

MESH = pl.DeviceIdType.MESH
EPSILON = 1e-06
BIG = 2.0**100
F32 = jnp.float32
BF16 = jnp.bfloat16

T = 512
L = 16
R = T + L
KEYS = 640
D = 1024
FF = 4096
CAP = 16
EXPERTS = 64
GROUPS = 4
FF_TILE = 512


def dot(a, b):
    return lax.dot_general(a, b, (((1,), (0,)), ((), ())), preferred_element_type=F32)


def dot_nt(a, b):
    return lax.dot_general(a, b, (((1,), (1,)), ((), ())), preferred_element_type=F32)


def norm_rows(rows, gain):
    mean = jnp.mean(rows, axis=-1, keepdims=True)
    centred = rows - mean
    spread = jnp.mean(centred * centred, axis=-1, keepdims=True)
    return centred * lax.rsqrt(spread + EPSILON) * gain


def column_of(row):
    eye = lax.broadcasted_iota(jnp.int32, (128, 128), 0) == lax.broadcasted_iota(
        jnp.int32, (128, 128), 1
    )
    pieces = []
    for i in range(row.shape[1] // 128):
        block = jnp.broadcast_to(row[:, i * 128 : (i + 1) * 128], (128, 128))
        pieces.append(jnp.sum(jnp.where(eye, block, 0.0), axis=1, keepdims=True))
    return jnp.concatenate(pieces, axis=0)


def layer_kernel(
    tok, lat, clip, eid, slot, g1, g2, router, wqkv_hbm, wout_hbm, fin_hbm, fout_hbm,
    out, newb,
    wqkv, wout, fin, fout, latx, normed, packed, qmask, kmask, attended, mid, expert_in,
    gate, disp, recv, outb, ret, acc, lat_send, lat_recv,
    wsem, dsend, drecv, rsend, rrecv, lsem,
):
    m = lax.axis_index("mod")
    e = lax.axis_index("exp")
    z = e // 16
    y = lax.rem(e // 8, 2)
    x = lax.rem(e // 2, 4)
    c = lax.rem(e, 2)
    me = z * 4 + y * 2 + c

    def partner(j, r, sign):
        oz = lax.rem(r, 4)
        zz = lax.rem(z + 4 + sign * oz, 4)
        xx = lax.rem(x + 8 + sign * (oz + j), 4)
        yy = lax.rem(y + lax.rem(r // 4, 2), 2)
        cc = lax.rem(c + r // 8, 2)
        return zz * 4 + yy * 2 + cc, zz * 16 + yy * 8 + xx * 2 + cc

    def places(i, j):
        zz = i // 64
        xx = lax.rem(x + 4 - z + zz + j, 4)
        return (zz * 16 + lax.rem(i // 32, 2) * 8 + xx * 2 + lax.rem(i // 16, 2)) * CAP + lax.rem(
            i, 16
        )

    qkv_copies = []
    for i in range(3):
        cols = pl.ds(i * D, D)
        cp = pltpu.make_async_copy(wqkv_hbm.at[0, :, cols], wqkv.at[:, cols], wsem.at[i])
        cp.start()
        qkv_copies.append(cp)
    out_copy = pltpu.make_async_copy(wout_hbm.at[0], wout, wsem.at[3])
    fin_copy = pltpu.make_async_copy(fin_hbm.at[0], fin, wsem.at[4])
    fout_copy = pltpu.make_async_copy(fout_hbm.at[0], fout, wsem.at[5])

    barrier = pltpu.get_barrier_semaphore()
    pl.semaphore_signal(barrier, inc=1, device_id=(1 - m, e), device_id_type=MESH)
    for g in range(GROUPS):

        def greet(r, carry, g=g):
            pl.semaphore_signal(
                barrier, inc=1, device_id=(m, partner(g, r, 1)[1]), device_id_type=MESH
            )
            return carry

        lax.fori_loop(1 if g == 0 else 0, 16, greet, 0)

    clip_start = e * 4
    lane = lax.broadcasted_iota(jnp.int32, (T, 128), 1)
    clip_col = column_of((clip[...] - clip_start).astype(F32)).astype(jnp.int32)
    hit = lane == clip_col
    qmask[0:T, :] = jnp.where(hit | (lane == 4), -BIG, 0.0).astype(BF16)
    kmask[0:T, :] = jnp.where(hit | (lane >= 4), 0.0, 1.0).astype(BF16)
    lane_l = lax.broadcasted_iota(jnp.int32, (L, 128), 1)
    clip_l = lax.broadcasted_iota(jnp.int32, (L, 128), 0) // 4
    hit_l = lane_l == clip_l
    qmask[T:R, :] = jnp.where(hit_l | (lane_l == 4), -BIG, 0.0).astype(BF16)
    kmask[T:R, :] = jnp.where(hit_l | (lane_l >= 4), 0.0, 1.0).astype(BF16)
    lane_p = lax.broadcasted_iota(jnp.int32, (KEYS - R, 128), 1)
    kmask[R:KEYS, :] = jnp.where(lane_p == 4, 1.0, 0.0).astype(BF16)
    packed[R:KEYS, :] = jnp.zeros((KEYS - R, 3 * D), BF16)

    gain1 = g1[...].astype(F32)

    def norm1(i, carry):
        rows = pl.ds(pl.multiple_of(i * 128, 128), 128)
        normed[rows, :] = norm_rows(tok[0, rows, :].astype(F32), gain1).astype(BF16)
        return carry

    lax.fori_loop(0, T // 128, norm1, 0)
    for i in range(4):
        latx[4 * i : 4 * i + 4, :] = lat[i].astype(F32)
    normed[T:R, :] = norm_rows(latx[...], gain1).astype(BF16)

    for i in range(3):
        qkv_copies[i].wait()
        if i == 0:
            out_copy.start()

        def project(j, carry, i=i):
            cols = pl.ds(pl.multiple_of(i * D + j * 512, 512), 512)
            piece = dot(normed[...], wqkv[:, cols]).astype(BF16)
            if i == 0:
                piece = piece * (1.0 / 8.0)
            packed[0:R, cols] = piece.astype(BF16)
            return carry

        lax.fori_loop(0, 2, project, 0)
    fin_copy.start()
    fout_copy.start()

    def pair(p, carry):
        col = pl.multiple_of(p * 128, 128)
        keys = jnp.concatenate([packed[:, pl.ds(D + col, 128)], kmask[...]], axis=1)
        values = jnp.concatenate(
            [packed[:, pl.ds(2 * D + col, 128)], jnp.ones((KEYS, 128), BF16)], axis=1
        )
        queries = packed[0:R, pl.ds(col, 128)]
        first = lax.broadcasted_iota(jnp.int32, (R, 128), 1) < 64
        heads = []
        for half in range(2):
            mine = jnp.where(first if half == 0 else ~first, queries, jnp.zeros_like(queries))
            q = jnp.concatenate([mine, qmask[...]], axis=1)
            s = dot_nt(q, keys)
            top = jnp.max(s, axis=-1, keepdims=True)
            w = jnp.exp(s - top).astype(BF16)
            o = dot(w, values)
            heads.append(o[:, :128] / o[:, 128:])
        attended[:, pl.ds(col, 128)] = jnp.where(first, heads[0], heads[1]).astype(BF16)
        return carry

    lax.fori_loop(0, D // 128, pair, 0)

    out_copy.wait()

    def project_out(j, carry):
        cols = pl.ds(pl.multiple_of(j * 512, 512), 512)
        mid[:, cols] = dot(attended[...], wout[:, cols])
        return carry

    lax.fori_loop(0, 2, project_out, 0)

    gain2 = g2[...].astype(F32)

    def norm2(i, carry):
        rows = pl.ds(pl.multiple_of(i * 128, 128), 128)
        updated = mid[rows, :] + tok[0, rows, :].astype(F32)
        mid[rows, :] = updated
        expert_in[rows, :] = norm_rows(updated, gain2).astype(BF16)
        return carry

    lax.fori_loop(0, T // 128, norm2, 0)
    lat_send[...] = (mid[T:R, :] + latx[...]).astype(BF16)

    pos_row = jnp.where(slot[...] < CAP, eid[...] * CAP + slot[...], -1)
    pl.semaphore_wait(barrier, 64)
    lat_copy = pltpu.make_async_remote_copy(
        src_ref=lat_send, dst_ref=lat_recv, send_sem=lsem.at[0], recv_sem=lsem.at[1],
        device_id=(1 - m, e), device_id_type=MESH,
    )
    lat_copy.start()
    for g in range(GROUPS):
        place = places(lax.broadcasted_iota(jnp.int32, (256, 1), 0), g)
        onehot = jnp.where(place == pos_row, 1.0, 0.0).astype(BF16)
        disp[g] = dot(onehot, expert_in[...]).astype(BF16).reshape(16, CAP, D)

        def send(r, carry, g=g):
            j, there = partner(g, r, 1)
            pltpu.make_async_remote_copy(
                src_ref=disp.at[g, j], dst_ref=recv.at[g, me],
                send_sem=dsend.at[g], recv_sem=drecv.at[g],
                device_id=(m, there), device_id_type=MESH,
            ).start()
            return carry

        lax.fori_loop(1 if g == 0 else 0, 16, send, 0)
    recv[0, me] = disp[0, me]

    logits = dot(expert_in[...], router[...])
    eid_col = column_of(eid[...].astype(F32)).astype(jnp.int32)
    expert_lane = lax.broadcasted_iota(jnp.int32, (T, EXPERTS), 1)
    picked = jnp.sum(jnp.where(expert_lane == eid_col, logits, 0.0), axis=1, keepdims=True)
    gate[...] = 1.0 / (1.0 + jnp.exp(-picked))
    pos_col = column_of(pos_row.astype(F32)).astype(jnp.int32)

    fin_copy.wait()
    fout_copy.wait()
    for g in range(GROUPS):
        n = 15 if g == 0 else 16
        landed = recv.at[g, pl.ds(0, n)]
        pltpu.make_async_copy(landed, landed, drecv.at[g]).wait()
        rows_in = recv[g].reshape(256, D)
        acc[...] = jnp.zeros_like(acc)

        def expert(f, carry, rows_in=rows_in):
            cols = pl.ds(pl.multiple_of(f * FF_TILE, FF_TILE), FF_TILE)
            h = dot(rows_in, fin[:, cols])
            h = (0.5 * h * (1.0 + lax.erf(h * math.sqrt(0.5)))).astype(BF16)
            acc[...] += dot(h, fout[cols, :])
            return carry

        lax.fori_loop(0, FF // FF_TILE, expert, 0)
        outb[g] = acc[...].astype(BF16).reshape(16, CAP, D)

        def send_back(r, carry, g=g):
            j, there = partner(g, r, -1)
            pltpu.make_async_remote_copy(
                src_ref=outb.at[g, j], dst_ref=ret.at[g, me],
                send_sem=rsend.at[g], recv_sem=rrecv.at[g],
                device_id=(m, there), device_id_type=MESH,
            ).start()
            return carry

        lax.fori_loop(1 if g == 0 else 0, 16, send_back, 0)
        if g == 0:
            ret[0, me] = outb[0, me]

    lat_copy.wait()
    both = (lat_send[...].astype(F32) + lat_recv[...].astype(F32)) * 0.5
    for i in range(4):
        newb[i] = both[4 * i : 4 * i + 4, :].astype(BF16)

    for g in range(GROUPS):
        n = 15 if g == 0 else 16
        landed = ret.at[g, pl.ds(0, n)]
        pltpu.make_async_copy(landed, landed, rrecv.at[g]).wait()
        place = places(lax.broadcasted_iota(jnp.int32, (1, 256), 1), g)
        onehot = jnp.where(place == pos_col, 1.0, 0.0).astype(BF16)
        total = mid[0:T, :] + gate[...] * dot(onehot, ret[g].reshape(256, D))
        if g < GROUPS - 1:
            mid[0:T, :] = total
        else:
            out[0] = total.astype(BF16)

    for g in range(GROUPS):
        n = 15 if g == 0 else 16
        sent = disp.at[g, pl.ds(0, n)]
        pltpu.make_async_copy(sent, sent, dsend.at[g]).wait()
        sent = outb.at[g, pl.ds(0, n)]
        pltpu.make_async_copy(sent, sent, rsend.at[g]).wait()


def on_device(
    tokens, bottleneck, clip_ids, expert_ids, slots, norm1_gain, attn_qkv, attn_out,
    norm2_gain, router, fc_in, fc_out,
):
    vmem = pl.BlockSpec(memory_space=pltpu.VMEM)
    hbm = pl.BlockSpec(memory_space=pl.ANY)
    dma = pltpu.SemaphoreType.DMA
    return pl.pallas_call(
        layer_kernel,
        out_shape=(
            jax.ShapeDtypeStruct(tokens.shape, BF16),
            jax.ShapeDtypeStruct(bottleneck.shape, BF16),
        ),
        in_specs=[vmem] * 8 + [hbm] * 4,
        out_specs=(vmem, vmem),
        scratch_shapes=[
            pltpu.VMEM((D, 3 * D), BF16),
            pltpu.VMEM((D, D), BF16),
            pltpu.VMEM((D, FF), BF16),
            pltpu.VMEM((FF, D), BF16),
            pltpu.VMEM((L, D), F32),
            pltpu.VMEM((R, D), BF16),
            pltpu.VMEM((KEYS, 3 * D), BF16),
            pltpu.VMEM((R, 128), BF16),
            pltpu.VMEM((KEYS, 128), BF16),
            pltpu.VMEM((R, D), BF16),
            pltpu.VMEM((R, D), F32),
            pltpu.VMEM((T, D), BF16),
            pltpu.VMEM((T, 1), F32),
            pltpu.VMEM((GROUPS, 16, CAP, D), BF16),
            pltpu.VMEM((GROUPS, 16, CAP, D), BF16),
            pltpu.VMEM((GROUPS, 16, CAP, D), BF16),
            pltpu.VMEM((GROUPS, 16, CAP, D), BF16),
            pltpu.VMEM((256, D), F32),
            pltpu.VMEM((L, D), BF16),
            pltpu.VMEM((L, D), BF16),
            dma((6,)),
            dma((GROUPS,)),
            dma((GROUPS,)),
            dma((GROUPS,)),
            dma((GROUPS,)),
            dma((2,)),
        ],
        compiler_params=pltpu.CompilerParams(
            collective_id=0, has_side_effects=True, vmem_limit_bytes=62 * 2**20
        ),
    )(
        tokens, bottleneck, clip_ids, expert_ids, slots, norm1_gain, norm2_gain, router,
        attn_qkv, attn_out, fc_in, fc_out,
    )


def solution(mesh):
    in_specs = (
        P("mod", "exp", None),
        P("exp", None, None),
        P("mod", "exp"),
        P("mod", "exp"),
        P("mod", "exp"),
        P("mod", None),
        P("mod", None, None),
        P("mod", None, None),
        P("mod", None),
        P(),
        P("exp", None, None),
        P("exp", None, None),
    )
    out_specs = (P("mod", "exp", None), P("exp", None, None))
    return jax.shard_map(
        on_device, mesh=mesh, in_specs=in_specs, out_specs=out_specs, check_vma=False
    )
```

```python
import functools
import math

import jax
import jax.numpy as jnp
from jax import lax
from jax.experimental import pallas as pl
from jax.experimental.pallas import tpu as pltpu
from jax.sharding import PartitionSpec as P

MESH = pl.DeviceIdType.MESH
EPSILON = 1e-06
BIG = 2.0**100
F32 = jnp.float32
BF16 = jnp.bfloat16

T = 512
L = 16
R = T + L
KEYS = 640
D = 1024
FF = 4096
CAP = 16
EXPERTS = 64
GROUPS = 4
FF_TILE = 1024
FIRST_SENT = 2
SENT_AFTER = {0: (2,), 1: (3,)}


def dot(a, b):
    return lax.dot_general(a, b, (((1,), (0,)), ((), ())), preferred_element_type=F32)


def dot_nt(a, b):
    return lax.dot_general(a, b, (((1,), (1,)), ((), ())), preferred_element_type=F32)


def norm_rows(rows, gain):
    mean = jnp.mean(rows, axis=-1, keepdims=True)
    centred = rows - mean
    spread = jnp.mean(centred * centred, axis=-1, keepdims=True)
    return centred * lax.rsqrt(spread + EPSILON) * gain


def column_of(row):
    eye = lax.broadcasted_iota(jnp.int32, (128, 128), 0) == lax.broadcasted_iota(
        jnp.int32, (128, 128), 1
    )
    pieces = []
    for i in range(row.shape[1] // 128):
        block = jnp.broadcast_to(row[:, i * 128 : (i + 1) * 128], (128, 128))
        pieces.append(jnp.sum(jnp.where(eye, block, 0.0), axis=1, keepdims=True))
    return jnp.concatenate(pieces, axis=0)


def layer_kernel(
    tok, lat, clip, eid, slot, g1, g2, router, wqkv_hbm, wout_hbm, fin_hbm, fout_hbm,
    out, newb,
    wqkv, wout, fin, fout, latx, normed, packed, qmask, kmask, attended, mid, expert_in,
    gate, disp, recv, outb, ret, hid, score, weight, act, lat_send, lat_recv,
    wsem, dsend, drecv, rsend, rrecv, lsem,
):
    m = lax.axis_index("mod")
    e = lax.axis_index("exp")
    z = e // 16
    y = lax.rem(e // 8, 2)
    x = lax.rem(e // 2, 4)
    c = lax.rem(e, 2)
    me = z * 4 + y * 2 + c

    def partner(j, r, sign):
        oz = lax.rem(r, 4)
        zz = lax.rem(z + 4 + sign * oz, 4)
        xx = lax.rem(x + 8 + sign * (oz + j), 4)
        yy = lax.rem(y + lax.rem(r // 4, 2), 2)
        cc = lax.rem(c + r // 8, 2)
        return zz * 4 + yy * 2 + cc, zz * 16 + yy * 8 + xx * 2 + cc

    def places(i, j):
        zz = i // 64
        xx = lax.rem(x + 4 - z + zz + j, 4)
        return (zz * 16 + lax.rem(i // 32, 2) * 8 + xx * 2 + lax.rem(i // 16, 2)) * CAP + lax.rem(
            i, 16
        )

    qkv_copies = []
    for i in range(3):
        cols = pl.ds(i * D, D)
        cp = pltpu.make_async_copy(wqkv_hbm.at[0, :, cols], wqkv.at[:, cols], wsem.at[i])
        cp.start()
        qkv_copies.append(cp)
    out_copy = pltpu.make_async_copy(wout_hbm.at[0], wout, wsem.at[3])
    fin_copy = pltpu.make_async_copy(fin_hbm.at[0], fin, wsem.at[4])
    fout_copy = pltpu.make_async_copy(fout_hbm.at[0], fout, wsem.at[5])

    barrier = pltpu.get_barrier_semaphore()
    pl.semaphore_signal(barrier, inc=1, device_id=(1 - m, e), device_id_type=MESH)
    for g in range(GROUPS):

        def greet(r, carry, g=g):
            pl.semaphore_signal(
                barrier, inc=1, device_id=(m, partner(g, r, 1)[1]), device_id_type=MESH
            )
            return carry

        lax.fori_loop(1 if g == 0 else 0, 16, greet, 0)

    clip_start = e * 4
    lane = lax.broadcasted_iota(jnp.int32, (T, 128), 1)
    clip_col = column_of((clip[...] - clip_start).astype(F32)).astype(jnp.int32)
    hit = lane == clip_col
    qmask[0:T, :] = jnp.where(hit | (lane == 4), -BIG, 0.0).astype(BF16)
    kmask[0:T, :] = jnp.where(hit | (lane >= 4), 0.0, 1.0).astype(BF16)
    lane_l = lax.broadcasted_iota(jnp.int32, (L, 128), 1)
    clip_l = lax.broadcasted_iota(jnp.int32, (L, 128), 0) // 4
    hit_l = lane_l == clip_l
    qmask[T:R, :] = jnp.where(hit_l | (lane_l == 4), -BIG, 0.0).astype(BF16)
    kmask[T:R, :] = jnp.where(hit_l | (lane_l >= 4), 0.0, 1.0).astype(BF16)
    lane_p = lax.broadcasted_iota(jnp.int32, (KEYS - R, 128), 1)
    kmask[R:KEYS, :] = jnp.where(lane_p == 4, 1.0, 0.0).astype(BF16)
    packed[R:KEYS, :] = jnp.zeros((KEYS - R, 3 * D), BF16)

    gain1 = g1[...].astype(F32)

    def norm1(i, carry):
        rows = pl.ds(pl.multiple_of(i * 128, 128), 128)
        normed[rows, :] = norm_rows(tok[0, rows, :].astype(F32), gain1).astype(BF16)
        return carry

    lax.fori_loop(0, T // 128, norm1, 0)
    for i in range(4):
        latx[4 * i : 4 * i + 4, :] = lat[i].astype(F32)
    normed[T:R, :] = norm_rows(latx[...], gain1).astype(BF16)

    for i in range(3):
        qkv_copies[i].wait()
        if i == 0:
            out_copy.start()

        def project(j, carry, i=i):
            cols = pl.ds(pl.multiple_of(i * D + j * 512, 512), 512)
            piece = dot(normed[...], wqkv[:, cols]).astype(BF16)
            if i == 0:
                piece = piece * (1.0 / 8.0)
            packed[0:R, cols] = piece.astype(BF16)
            return carry

        lax.fori_loop(0, 2, project, 0)
    fin_copy.start()
    fout_copy.start()

    def pair(p, carry):
        col = pl.multiple_of(p * 128, 128)
        keys = jnp.concatenate([packed[:, pl.ds(D + col, 128)], kmask[...]], axis=1)
        values = jnp.concatenate(
            [packed[:, pl.ds(2 * D + col, 128)], jnp.ones((KEYS, 128), BF16)], axis=1
        )
        queries = packed[0:R, pl.ds(col, 128)]
        first = lax.broadcasted_iota(jnp.int32, (R, 128), 1) < 64
        heads = []
        for half in range(2):
            mine = jnp.where(first if half == 0 else ~first, queries, jnp.zeros_like(queries))
            q = jnp.concatenate([mine, qmask[...]], axis=1)
            score[half] = dot_nt(q, keys)
        for half in range(2):
            for row0 in range(0, R, 48):
                s = score[half, row0 : row0 + 48, :]
                top = jnp.max(s, axis=-1, keepdims=True)
                weight[half, row0 : row0 + 48, :] = jnp.exp(s - top).astype(BF16)
            o = dot(weight[half], values)
            heads.append(o[:, :128] / o[:, 128:])
        attended[:, pl.ds(col, 128)] = jnp.where(first, heads[0], heads[1]).astype(BF16)
        return carry

    lax.fori_loop(0, D // 128, pair, 0)

    out_copy.wait()

    def project_out(j, carry):
        cols = pl.ds(pl.multiple_of(j * 512, 512), 512)
        mid[:, cols] = dot(attended[...], wout[:, cols])
        return carry

    lax.fori_loop(0, 2, project_out, 0)

    gain2 = g2[...].astype(F32)

    def norm2(i, carry):
        rows = pl.ds(pl.multiple_of(i * 128, 128), 128)
        updated = mid[rows, :] + tok[0, rows, :].astype(F32)
        mid[rows, :] = updated
        expert_in[rows, :] = norm_rows(updated, gain2).astype(BF16)
        return carry

    lax.fori_loop(0, T // 128, norm2, 0)
    lat_send[...] = (mid[T:R, :] + latx[...]).astype(BF16)

    pos_row = jnp.where(slot[...] < CAP, eid[...] * CAP + slot[...], -1)
    pl.semaphore_wait(barrier, 64)
    lat_copy = pltpu.make_async_remote_copy(
        src_ref=lat_send, dst_ref=lat_recv, send_sem=lsem.at[0], recv_sem=lsem.at[1],
        device_id=(1 - m, e), device_id_type=MESH,
    )
    lat_copy.start()
    def dispatch(g):
        def send(r, carry):
            j, there = partner(g, r, 1)
            pltpu.make_async_remote_copy(
                src_ref=disp.at[g, j], dst_ref=recv.at[g, me],
                send_sem=dsend.at[g], recv_sem=drecv.at[g],
                device_id=(m, there), device_id_type=MESH,
            ).start()
            return carry

        lax.fori_loop(1 if g == 0 else 0, 16, send, 0)

    for g in range(GROUPS):
        place = places(lax.broadcasted_iota(jnp.int32, (256, 1), 0), g)
        onehot = jnp.where(place == pos_row, 1.0, 0.0).astype(BF16)
        disp[g] = dot(onehot, expert_in[...]).astype(BF16).reshape(16, CAP, D)
        if g < FIRST_SENT:
            dispatch(g)
    recv[0, me] = disp[0, me]

    logits = dot_nt(expert_in[...], router[...])
    eid_col = column_of(eid[...].astype(F32)).astype(jnp.int32)
    expert_lane = lax.broadcasted_iota(jnp.int32, (T, EXPERTS), 1)
    picked = jnp.sum(jnp.where(expert_lane == eid_col, logits, 0.0), axis=1, keepdims=True)
    gate[...] = 1.0 / (1.0 + jnp.exp(-picked))
    pos_col = column_of(pos_row.astype(F32)).astype(jnp.int32)

    fin_copy.wait()
    fout_copy.wait()
    for g in range(GROUPS):
        n = 15 if g == 0 else 16
        landed = recv.at[g, pl.ds(0, n)]
        pltpu.make_async_copy(landed, landed, drecv.at[g]).wait()
        for later in SENT_AFTER.get(g, ()):
            dispatch(later)

        def activate(f, slot):
            h = hid[slot]
            h = 0.5 * h * (1.0 + lax.erf(h * math.sqrt(0.5)))
            act[:, pl.ds(pl.multiple_of(f * FF_TILE, FF_TILE), FF_TILE)] = h.astype(BF16)

        def first_layer(f, slot):
            hid[slot] = dot(
                recv[g].reshape(256, D),
                fin[:, pl.ds(pl.multiple_of(f * FF_TILE, FF_TILE), FF_TILE)],
            )

        first_layer(0, 0)

        def expert(i, carry):
            first_layer(2 * i + 1, 1)
            activate(2 * i, 0)
            first_layer(2 * i + 2, 0)
            activate(2 * i + 1, 1)
            return carry

        lax.fori_loop(0, FF // FF_TILE // 2 - 1, expert, 0)
        first_layer(FF // FF_TILE - 1, 1)
        activate(FF // FF_TILE - 2, 0)
        activate(FF // FF_TILE - 1, 1)

        def second_layer(f, carry, g=g):
            cols = pl.ds(pl.multiple_of(f * 256, 256), 256)
            outb[g, :, :, cols] = dot(act[...], fout[:, cols]).astype(BF16).reshape(16, CAP, 256)
            return carry

        lax.fori_loop(0, D // 256, second_layer, 0)

        def send_back(r, carry, g=g):
            j, there = partner(g, r, -1)
            pltpu.make_async_remote_copy(
                src_ref=outb.at[g, j], dst_ref=ret.at[g, me],
                send_sem=rsend.at[g], recv_sem=rrecv.at[g],
                device_id=(m, there), device_id_type=MESH,
            ).start()
            return carry

        lax.fori_loop(1 if g == 0 else 0, 16, send_back, 0)
        if g == 0:
            ret[0, me] = outb[0, me]

    lat_copy.wait()
    both = (lat_send[...].astype(F32) + lat_recv[...].astype(F32)) * 0.5
    for i in range(4):
        newb[i] = both[4 * i : 4 * i + 4, :].astype(BF16)

    for g in range(GROUPS):
        n = 15 if g == 0 else 16
        landed = ret.at[g, pl.ds(0, n)]
        pltpu.make_async_copy(landed, landed, rrecv.at[g]).wait()
        place = places(lax.broadcasted_iota(jnp.int32, (1, 256), 1), g)
        onehot = jnp.where(place == pos_col, 1.0, 0.0).astype(BF16)
        total = mid[0:T, :] + gate[...] * dot(onehot, ret[g].reshape(256, D))
        if g < GROUPS - 1:
            mid[0:T, :] = total
        else:
            out[0] = total.astype(BF16)

    for g in range(GROUPS):
        n = 15 if g == 0 else 16
        sent = disp.at[g, pl.ds(0, n)]
        pltpu.make_async_copy(sent, sent, dsend.at[g]).wait()
        sent = outb.at[g, pl.ds(0, n)]
        pltpu.make_async_copy(sent, sent, rsend.at[g]).wait()


def on_device(
    tokens, bottleneck, clip_ids, expert_ids, slots, norm1_gain, attn_qkv, attn_out,
    norm2_gain, router, fc_in, fc_out,
):
    vmem = pl.BlockSpec(memory_space=pltpu.VMEM)
    hbm = pl.BlockSpec(memory_space=pl.ANY)
    dma = pltpu.SemaphoreType.DMA
    return pl.pallas_call(
        layer_kernel,
        out_shape=(
            jax.ShapeDtypeStruct(tokens.shape, BF16),
            jax.ShapeDtypeStruct(bottleneck.shape, BF16),
        ),
        in_specs=[vmem] * 8 + [hbm] * 4,
        out_specs=(vmem, vmem),
        scratch_shapes=[
            pltpu.VMEM((D, 3 * D), BF16),
            pltpu.VMEM((D, D), BF16),
            pltpu.VMEM((D, FF), BF16),
            pltpu.VMEM((FF, D), BF16),
            pltpu.VMEM((L, D), F32),
            pltpu.VMEM((R, D), BF16),
            pltpu.VMEM((KEYS, 3 * D), BF16),
            pltpu.VMEM((R, 128), BF16),
            pltpu.VMEM((KEYS, 128), BF16),
            pltpu.VMEM((R, D), BF16),
            pltpu.VMEM((R, D), F32),
            pltpu.VMEM((T, D), BF16),
            pltpu.VMEM((T, 1), F32),
            pltpu.VMEM((GROUPS, 16, CAP, D), BF16),
            pltpu.VMEM((GROUPS, 16, CAP, D), BF16),
            pltpu.VMEM((GROUPS, 16, CAP, D), BF16),
            pltpu.VMEM((GROUPS, 16, CAP, D), BF16),
            pltpu.VMEM((2, 256, FF_TILE), F32),
            pltpu.VMEM((2, R, KEYS), F32),
            pltpu.VMEM((2, R, KEYS), BF16),
            pltpu.VMEM((256, FF), BF16),
            pltpu.VMEM((L, D), BF16),
            pltpu.VMEM((L, D), BF16),
            dma((6,)),
            dma((GROUPS,)),
            dma((GROUPS,)),
            dma((GROUPS,)),
            dma((GROUPS,)),
            dma((2,)),
        ],
        compiler_params=pltpu.CompilerParams(
            collective_id=0, has_side_effects=True, vmem_limit_bytes=62 * 2**20
        ),
    )(
        tokens, bottleneck, clip_ids, expert_ids, slots, norm1_gain, norm2_gain, router.T,
        attn_qkv, attn_out, fc_in, fc_out,
    )


def solution(mesh):
    in_specs = (
        P("mod", "exp", None),
        P("exp", None, None),
        P("mod", "exp"),
        P("mod", "exp"),
        P("mod", "exp"),
        P("mod", None),
        P("mod", None, None),
        P("mod", None, None),
        P("mod", None),
        P(),
        P("exp", None, None),
        P("exp", None, None),
    )
    out_specs = (P("mod", "exp", None), P("exp", None, None))
    return jax.shard_map(
        on_device, mesh=mesh, in_specs=in_specs, out_specs=out_specs, check_vma=False
    )
```
